32 devices in a mesh: row: 8 (over y, x, core), col: 4 (over z).
Axes of the slice: x: 2, y: 2, z: 4, core: 2. Of those that a mesh axis runs over, the one named last changes fastest.
Arguments:
- right_side: float32 [2, 2048, 1024], P(None, 'row', 'col'), may hold values from -6 to 6
- probe: float32 [2, 256, 256], replicated, may hold values from -6 to 6
- detector_weights: float32 [256, 256], replicated, may hold values from 0.1 to 10
- offsets: int32 [8, 4, 4, 2], P('row', 'col'), may hold values from -128 to 127, as said below
- counts: int32 [8, 4], P('row', 'col'), may hold values from 2 to 4, as said below
Outputs:
- solution_field: float32 [2, 2048, 1024], P(None, 'row', 'col')
- residual: float32 [2, 2048, 1024], P(None, 'row', 'col')
The draws below stay inside these ranges and needn't reach their ends.
Inputs may be any that keep to these rules, and one draw needn't show every extreme that they name: `counts`: every region holds at least two positions; in every draw some region holds exactly 4. In every region slot 0 has both offsets negative and slot 1 both offsets non-negative.
All inputs are finite; a program needn't handle non-finite values.
Results may differ from the reference program's by a relative error of at most 0.0003.
Values sent between devices are 32-bit elements; how exact they have to be, the bound alone decides.
A program may use at most 64 MiB of HBM per device.

```python
import math
import jax
import jax.numpy as jnp
from jax import lax

PATCH = 256
CAP = 4
ITERS = 3
NY = 2048
NX = 1024
N_ROW = 8
N_COL = 4


def draw_counts(key, part):
    key_full, key_low, key_pick = jax.random.split(jax.random.fold_in(key, 71), 3)
    heavy = jax.random.randint(key_full, (N_ROW, N_COL), 0, 4) == 0
    light = jax.random.randint(key_low, (N_ROW, N_COL), 2, max(CAP // 2, 2) + 1)
    filled = jnp.where(heavy, CAP, light).reshape(-1)
    chosen = jax.random.randint(key_pick, (), 0, N_ROW * N_COL)
    filled = filled.at[chosen].set(CAP)
    return filled.reshape(N_ROW, N_COL).astype(jnp.int32)


def draw_offsets(key, part):
    half = PATCH // 2
    key_rest, key_low, key_high = jax.random.split(jax.random.fold_in(key, 53), 3)
    rest = jax.random.randint(key_rest, (N_ROW, N_COL, CAP, 2), -half, half)
    low = jax.random.randint(key_low, (N_ROW, N_COL, 1, 2), -half, 0)
    high = jax.random.randint(key_high, (N_ROW, N_COL, 1, 2), 0, half)
    return jnp.concatenate([low, high, rest[:, :, 2:]], axis=2).astype(jnp.int32)


def shard_levels(stream_key, extent, shards, least, high):
    def one(position, blocks):
        draws = jax.random.uniform(jax.random.fold_in(jax.random.fold_in(stream_key, 6), position), (blocks,), jnp.float32, least / len(shards), high / len(shards))
        return jnp.repeat(jnp.exp(draws), extent[position] // blocks).reshape((-1,) + (1,) * (len(extent) - position - 1))

    gain = one(*shards[0])
    for cut in shards[1:]:
        gain = gain * one(*cut)
    return gain


def centred(own_key, shape, spread, bound, cuts=(), held_as=jnp.bfloat16):
    drawn = jax.random.normal(own_key, shape, jnp.float32) * spread
    if len(cuts) > 0:
        drawn = shard_levels(own_key, shape, cuts, -0.22, 0.18) * drawn
    return jnp.clip(drawn, min=-bound, max=bound).astype(held_as)


def setup_inputs(seed: int = 0) -> dict:
    arg_keys = jax.random.split(jax.random.key(seed), 6)
    return {
        "right_side": centred(arg_keys[0], (2, NY, NX), 1.0, 6.0, ((1, 8), (2, 4)), jnp.float32),
        "probe": centred(arg_keys[1], (2, PATCH, PATCH), 1.0, 6.0, (), jnp.float32),
        "detector_weights": jnp.clip(jnp.exp(jax.random.uniform(arg_keys[2], (PATCH, PATCH), jnp.float32, math.log(0.1), math.log(10.0))), 0.1, 10.0),
        "offsets": draw_offsets(jax.random.fold_in(arg_keys[5], 71), 0),
        "counts": draw_counts(jax.random.fold_in(arg_keys[5], 71), 0),
    }


ridge_weight = 0.5


def patch_normal(tile_in, probe, weights):
    illum = lax.complex(probe[0], probe[1])
    wave = illum * lax.complex(tile_in[0], tile_in[1])
    freq = jnp.fft.fft2(wave, norm="ortho")
    back = jnp.fft.ifft2(freq * weights, norm="ortho")
    result = jnp.conj(illum) * back
    return jnp.stack([jnp.real(result), jnp.imag(result)])


def operate(field, probe, weights, row_starts, col_starts, weight_on):
    margin = PATCH // 2
    padded = jnp.pad(field, ((0, 0), (margin, margin), (margin, margin)))

    def visit(summed, item):
        row_at, col_at, flag = item
        zero_idx = jnp.zeros((), jnp.int32)
        tile_in = lax.dynamic_slice(padded, (zero_idx, row_at, col_at), (2, PATCH, PATCH))
        update = patch_normal(tile_in, probe, weights) * flag
        current = lax.dynamic_slice(summed, (zero_idx, row_at, col_at), (2, PATCH, PATCH))
        return lax.dynamic_update_slice(summed, current + update, (zero_idx, row_at, col_at)), None

    summed, _ = lax.scan(visit, jnp.zeros_like(padded), (row_starts, col_starts, weight_on))
    return summed[:, margin:margin + NY, margin:margin + NX] + ridge_weight * field


def inner(first, second):
    return jnp.sum(first * second)


def reference(right_side, probe, detector_weights, offsets, counts):
    margin = PATCH // 2
    region_row = (jnp.arange(N_ROW, dtype=jnp.int32) * PATCH + margin)[:, None, None]
    region_col = (jnp.arange(N_COL, dtype=jnp.int32) * PATCH + margin)[None, :, None]
    row_starts = (offsets[:, :, :, 0].astype(jnp.int32) + region_row).reshape(-1).astype(jnp.int32)
    col_starts = (offsets[:, :, :, 1].astype(jnp.int32) + region_col).reshape(-1).astype(jnp.int32)
    slot_ids = jnp.arange(CAP, dtype=jnp.int32)[None, None, :]
    weight_on = (slot_ids < counts[:, :, None]).astype(jnp.float32).reshape(-1)
    solution_field = jnp.zeros_like(right_side)
    residual, direction = right_side, right_side
    norm_now = inner(residual, residual)
    for iteration in range(ITERS):
        image = operate(direction, probe, detector_weights, row_starts, col_starts, weight_on)
        alpha = norm_now / inner(direction, image)
        solution_field = solution_field + alpha * direction
        residual = residual - alpha * image
        norm_next = inner(residual, residual)
        direction = residual + (norm_next / norm_now) * direction
        norm_now = norm_next
    return solution_field, residual
```

```python
import math

import jax
import jax.numpy as jnp
from jax import lax
from jax.sharding import PartitionSpec as P

ITERS = 3


ridge_weight = 0.5
highest = lax.Precision.HIGH


def extended(block, sides, width):
    for axis, dim in sides:
        count = lax.axis_size(axis)
        forward = [(i, i + 1) for i in range(count - 1)]
        backward = [(target, source) for source, target in forward]
        low = lax.ppermute(
            lax.slice_in_dim(block, block.shape[dim] - width, None, axis=dim), axis, forward
        )
        high = lax.ppermute(lax.slice_in_dim(block, 0, width, axis=dim), axis, backward)
        block = jnp.concatenate([low, block, high], axis=dim)
    return block


def passed_along(value, axis, steps):
    count = lax.axis_size(axis)
    first, last = (max(0, -steps), min(count, count - steps))
    return lax.ppermute(value, axis, [(source, source + steps) for source in range(first, last)])


def matmul(left, right):
    return jnp.dot(left, right, precision=highest)


def tables(length):
    ramp = lax.iota(jnp.int32, length)
    phase = ramp[:, None] * ramp[None, :] % length
    angle = phase.astype(jnp.float32) * (2.0 * math.pi / length)
    norm_scale = 1.0 / math.sqrt(length)
    return (jnp.cos(angle) * norm_scale, -jnp.sin(angle) * norm_scale)


def complex_left(mat_re, mat_im, arg_re, arg_im):
    return (
        matmul(mat_re, arg_re) - matmul(mat_im, arg_im),
        matmul(mat_re, arg_im) + matmul(mat_im, arg_re),
    )


def complex_right(arg_re, arg_im, mat_re, mat_im):
    return (
        matmul(arg_re, mat_re) - matmul(arg_im, mat_im),
        matmul(arg_re, mat_im) + matmul(arg_im, mat_re),
    )


def transform(arg_re, arg_im, mat_re, mat_im):
    first_re, first_im = complex_left(mat_re, mat_im, arg_re, arg_im)
    return complex_right(first_re, first_im, mat_re, mat_im)


def patch_normal(tile_in, probe, weights, mat_re, mat_im):
    probe_re, probe_im = (probe[0], probe[1])
    wave_re = probe_re * tile_in[0] - probe_im * tile_in[1]
    wave_im = probe_re * tile_in[1] + probe_im * tile_in[0]
    freq_re, freq_im = transform(wave_re, wave_im, mat_re, mat_im)
    back_re, back_im = transform(weights * freq_re, weights * freq_im, mat_re, -mat_im)
    return jnp.stack(
        [probe_re * back_re + probe_im * back_im, probe_re * back_im - probe_im * back_re]
    )


def operate(field, probe, weights, offsets, counts, mat_re, mat_im):
    side = field.shape[1]
    margin = side // 2
    window = extended(field, (("row", 1), ("col", 2)), margin)
    filled = counts[0, 0]

    def visit(slot_idx, summed):
        row_at = offsets[0, 0, slot_idx, 0] + margin
        col_at = offsets[0, 0, slot_idx, 1] + margin
        zero_idx = jnp.zeros((), jnp.int32)
        tile_in = lax.dynamic_slice(window, (zero_idx, row_at, col_at), (2, side, side))
        weight_on = (slot_idx < filled).astype(jnp.float32)
        update = patch_normal(tile_in, probe, weights, mat_re, mat_im) * weight_on
        current = lax.dynamic_slice(summed, (zero_idx, row_at, col_at), (2, side, side))
        return lax.dynamic_update_slice(summed, current + update, (zero_idx, row_at, col_at))

    summed = jnp.zeros((2, 2 * side, 2 * side), jnp.float32)
    upper = offsets.shape[2]
    summed = lax.fori_loop(0, upper, visit, summed)
    from_above = passed_along(summed[:, margin + side :, :], "row", 1)
    from_below = passed_along(summed[:, :margin, :], "row", -1)
    middle = summed[:, margin : margin + side, :] + jnp.concatenate(
        [from_above, from_below], axis=1
    )
    from_left = passed_along(middle[:, :, margin + side :], "col", 1)
    from_right = passed_along(middle[:, :, :margin], "col", -1)
    centre = middle[:, :, margin : margin + side] + jnp.concatenate([from_left, from_right], axis=2)
    return centre + ridge_weight * field


def inner(first, second):
    return jnp.sum(first * second)


def two_products(residual, image):
    return lax.psum((inner(residual, residual), inner(residual, image)), ("row", "col"))


def local(right_side, probe, detector_weights, offsets, counts):
    mat_re, mat_im = tables(probe.shape[1])

    def apply_op(field):
        return operate(field, probe, detector_weights, offsets, counts, mat_re, mat_im)

    solution_field = jnp.zeros_like(right_side)
    residual = right_side
    image = apply_op(residual)
    norm_now, product = two_products(residual, image)
    alpha = norm_now / product
    direction, along = (residual, image)
    for iteration in range(ITERS):
        solution_field = solution_field + alpha * direction
        residual = residual - alpha * along
        if iteration + 1 < ITERS:
            image = apply_op(residual)
            norm_next, product = two_products(residual, image)
            ratio = norm_next / norm_now
            alpha = norm_next / (product - ratio * norm_next / alpha)
            direction = residual + ratio * direction
            along = image + ratio * along
            norm_now = norm_next
    return (solution_field, residual)


def solution(mesh):
    placed = (P(None, "row", "col"), P(), P(), P("row", "col", None, None), P("row", "col"))
    return jax.shard_map(
        local,
        mesh=mesh,
        in_specs=placed,
        out_specs=(P(None, "row", "col"), P(None, "row", "col")),
        check_vma=False,
    )
```

```python
import functools
import math

import jax
import jax.numpy as jnp
import numpy as np
from jax import lax
from jax.experimental import pallas as pl
from jax.experimental.pallas import tpu as pltpu
from jax.sharding import PartitionSpec as P

ITERS = 3
RIDGE = 0.5
MESH = pl.DeviceIdType.MESH
F32 = jnp.float32
BF16 = jnp.bfloat16


def tables(length):
    half = length // 2
    k = np.arange(half)[:, None]
    n = np.arange(half)[None, :]
    out = []
    for odd in (0, 1):
        angle = 2.0 * math.pi * ((n * (2 * k + odd)) % length) / length
        re, im = np.cos(angle) / math.sqrt(length), -np.sin(angle) / math.sqrt(length)
        real = np.block([[re, -im], [im, re]])
        for mat in (real, real.T):
            hi = mat.astype(BF16)
            out += [hi, (mat - hi.astype(np.float64)).astype(BF16)]
    return np.stack(out)


def kernel(
    n_row, n_col, cap, side,
    off_ref, cnt_ref, rhs_ref, probe_ref, w_ref, mat_ref,
    sol_ref, res_ref,
    R, G, L, S, D, PR, X, Y, RB, CB, T, T1, T2,
    bar_send, bar_recv, s1_send, s1_recv, s2_send, s2_recv,
):
    h = side // 2
    own = slice(h, h + side)
    row = lax.axis_index("row")
    col = lax.axis_index("col")

    def chunks(total, step, body):
        def run(i, carry):
            body(pl.ds(pl.multiple_of(i * step, step), step), i * step)
            return carry
        lax.fori_loop(0, total // step, run, 0)

    def clear(rows, _):
        G[:, rows, :] = jnp.zeros((2, 32, 2 * side), F32)
    chunks(2 * side, 32, clear)

    def clear_b(rows, _):
        RB[:, :, rows, :] = jnp.zeros((2, 2, 32, 2 * side), F32)
    chunks(h, 32, clear_b)

    def clear_c(rows, _):
        CB[:, :, rows, :] = jnp.zeros((2, 2, 32, h), F32)
    chunks(side, 32, clear_c)
    G[:, own, own] = rhs_ref[...]

    barrier = pltpu.get_barrier_semaphore()
    for d in range(1, n_row):
        pl.semaphore_signal(barrier, inc=1, device_id=(lax.rem(row + d, n_row), col), device_id_type=MESH)
    for d in range(1, n_col):
        pl.semaphore_signal(barrier, inc=1, device_id=(row, lax.rem(col + d, n_col)), device_id_type=MESH)
    pl.semaphore_wait(barrier, n_row - 1 + n_col - 1)

    def both(index, low_src, low_dst, high_src, high_dst, axis):
        at, count = (row, n_row) if axis == 0 else (col, n_col)

        def target(step):
            return (row + step, col) if axis == 0 else (row, col + step)

        low = pltpu.make_async_remote_copy(
            src_ref=low_src, dst_ref=low_dst, send_sem=bar_send.at[2 * index], recv_sem=bar_recv.at[2 * index],
            device_id=target(-1), device_id_type=MESH)
        high = pltpu.make_async_remote_copy(
            src_ref=high_src, dst_ref=high_dst, send_sem=bar_send.at[2 * index + 1],
            recv_sem=bar_recv.at[2 * index + 1], device_id=target(1), device_id_type=MESH)

        def start():
            pl.when(at > 0)(low.start)
            pl.when(at < count - 1)(high.start)

        def wait():
            @pl.when(at > 0)
            def _():
                low.wait_send()
                high.wait_recv()

            @pl.when(at < count - 1)
            def _():
                high.wait_send()
                low.wait_recv()

        return start, wait

    def gather():
        start, wait = both(
            2, G.at[:, own, h:2 * h], G.at[:, own, 3 * h:4 * h], G.at[:, own, 2 * h:3 * h], G.at[:, own, 0:h], 1)
        start()
        wait()
        start, wait = both(
            3, G.at[:, h:2 * h, :], G.at[:, 3 * h:4 * h, :], G.at[:, 2 * h:3 * h, :], G.at[:, 0:h, :], 0)
        start()
        return wait

    gather_wait = gather()

    for s in range(cap):
        on = jnp.where(s < cnt_ref[0], 1.0, 0.0).astype(F32)
        for c in range(2):
            rolled = pltpu.roll(probe_ref[c], off_ref[2 * s] + h, 0)
            PR[s, c] = pltpu.roll(rolled, off_ref[2 * s + 1] + h, 1) * on

    gather_wait()

    def put(j, rows, val):
        hi = val.astype(BF16)
        X[j, 0, rows, :] = hi
        X[j, 1, rows, :] = (val - hi.astype(F32)).astype(BF16)

    def left(m, j):
        hi, lo = mat_ref[m], mat_ref[m + 1]
        xh, xl = X[j, 0], X[j, 1]
        return jnp.dot(jnp.concatenate([hi, lo, hi], 1), jnp.concatenate([xh, xh, xl], 0), preferred_element_type=F32)

    def right(j, m):
        hi, lo = mat_ref[m], mat_ref[m + 1]
        xh, xl = X[j, 0], X[j, 1]
        return jnp.dot(jnp.concatenate([xh, xl, xh], 1), jnp.concatenate([hi, hi, lo], 0), preferred_element_type=F32)

    step = 32

    def fold(val):
        return jnp.sum(val.reshape(-1, 8, val.shape[-1]), axis=0)

    def patch(s, acc):
        a = off_ref[2 * s] + h
        b = off_ref[2 * s + 1] + h
        ri = lax.broadcasted_iota(jnp.int32, (step, side), 0)
        in_col = lax.broadcasted_iota(jnp.int32, (step, side), 1) >= b
        for t in range(0, h, step):
            parts = []
            for base in (t, h + t):
                rows, far = slice(base, base + step), slice(side + base, side + base + step)
                in_row = ri + base >= a
                v = [
                    jnp.where(in_row, jnp.where(in_col, R[c, rows, 0:side], R[c, rows, side:]),
                              jnp.where(in_col, R[c, far, 0:side], R[c, far, side:]))
                    for c in range(2)
                ]
                p0, p1 = PR[s, 0, rows, :], PR[s, 1, rows, :]
                parts.append((p0 * v[0] - p1 * v[1], p0 * v[1] + p1 * v[0]))
            for c in range(2):
                rows = slice(c * h + t, c * h + t + step)
                put(0, rows, parts[0][c] + parts[1][c])
                put(1, rows, parts[0][c] - parts[1][c])
        Y[0] = left(0, 0)
        Y[1] = left(4, 1)
        for j in range(2):
            for t in range(0, h, step):
                re, im = Y[j, t:t + step, :], Y[j, h + t:h + t + step, :]
                rows = slice(j * h + t, j * h + t + step)
                put(2, rows, jnp.concatenate([re[:, :h] + re[:, h:], im[:, :h] + im[:, h:]], 1))
                put(3, rows, jnp.concatenate([re[:, :h] - re[:, h:], im[:, :h] - im[:, h:]], 1))
        Y[2] = right(2, 2)
        Y[3] = right(3, 6)
        for j in range(2):
            for t in range(0, side, step):
                rows = slice(t, t + step)
                f = Y[2 + j, rows, :]
                wf = w_ref[j, rows, :] * f
                acc = acc + fold(wf * f)
                put(j, rows, wf)
        Y[0] = right(0, 0)
        Y[1] = right(1, 4)
        for j in range(2):
            for t in range(0, h, step):
                rows = slice(j * h + t, j * h + t + step)
                c, d = Y[0, rows, :], Y[1, rows, :]
                p, m = c + d, c - d
                put(2 + j, slice(t, t + step), jnp.concatenate([p[:, :h], m[:, :h]], 1))
                put(2 + j, slice(h + t, h + t + step), jnp.concatenate([p[:, h:], m[:, h:]], 1))
        Y[2] = left(2, 2)
        Y[3] = left(6, 3)
        for t in range(0, h, step):
            for sign, base in ((1, t), (-1, h + t)):
                rows, far = slice(base, base + step), slice(side + base, side + base + step)
                hr = Y[2, t:t + step, :] + sign * Y[3, t:t + step, :]
                hi = Y[2, h + t:h + t + step, :] + sign * Y[3, h + t:h + t + step, :]
                p0, p1 = PR[s, 0, rows, :], PR[s, 1, rows, :]
                in_row = ri + base >= a
                for c, term in ((0, p0 * hr + p1 * hi), (1, p0 * hi - p1 * hr)):
                    near_r = jnp.where(in_row, term, 0.0)
                    far_r = term - near_r
                    nn = jnp.where(in_col, near_r, 0.0)
                    fn = jnp.where(in_col, far_r, 0.0)
                    S[c, rows, 0:side] += nn
                    S[c, rows, side:] += near_r - nn
                    S[c, far, 0:side] += fn
                    S[c, far, side:] += far_r - fn
        return acc

    def copy_r(rows, _):
        R[:, rows, :] = G[:, rows, :]
    chunks(2 * side, 32, copy_r)

    ti = lax.broadcasted_iota(jnp.int32, (8, 128), 0)

    def lanes(acc):
        total = acc[:, 0:128]
        for q in range(128, acc.shape[1], 128):
            total = total + acc[:, q:q + 128]
        return jnp.sum(total, axis=0, keepdims=True)

    alpha = rr_before = None
    for it in range(ITERS):
        last = it + 1 == ITERS

        def clear_s(rows, _):
            S[:, rows, :] = jnp.zeros((2, 32, 2 * side), F32)
        chunks(2 * side, 32, clear_s)

        def norm(i, acc):
            v = R[:, pl.ds(pl.multiple_of(h + i * 32, 32), 32), own]
            return acc + fold(v[0] * v[0]) + fold(v[1] * v[1])
        rr_acc = lax.fori_loop(0, side // 32, norm, jnp.zeros((8, side), F32))
        acc = lax.fori_loop(0, cap, patch, jnp.zeros((8, side), F32))

        rs_start, rs_wait = both(0, S.at[:, 0:h, :], RB.at[0], S.at[:, 3 * h:4 * h, :], RB.at[1], 0)
        rs_start()
        rr_l, pap_l = lanes(rr_acc), lanes(acc)
        T1[it, row] = jnp.where(ti == 0, rr_l, jnp.where(ti == 1, pap_l + RIDGE * rr_l, 0.0))
        ones = [
            pltpu.make_async_remote_copy(
                src_ref=T1.at[it, row], dst_ref=T1.at[it, row], send_sem=s1_send.at[it, d],
                recv_sem=s1_recv.at[it, d], device_id=(lax.rem(row + d, n_row), col), device_id_type=MESH)
            for d in range(1, n_row)
        ]
        for copy in ones:
            copy.start()
        rs_wait()

        def add_rows(i, carry):
            near = pl.ds(pl.multiple_of(i * 32, 32), 32)
            top = pl.ds(pl.multiple_of(h + i * 32, 32), 32)
            bottom = pl.ds(pl.multiple_of(2 * h + i * 32, 32), 32)
            S[:, top, :] += RB[1, :, near, :]
            S[:, bottom, :] += RB[0, :, near, :]
            return carry
        lax.fori_loop(0, h // 32, add_rows, 0)
        cs_start, cs_wait = both(1, S.at[:, own, 0:h], CB.at[0], S.at[:, own, 3 * h:4 * h], CB.at[1], 1)
        cs_start()
        for copy in ones:
            copy.wait()
        total = T1[it, 0]
        for q in range(1, n_row):
            total = total + T1[it, q]
        T2[it, col] = total
        twos = [
            pltpu.make_async_remote_copy(
                src_ref=T2.at[it, col], dst_ref=T2.at[it, col], send_sem=s2_send.at[it, d],
                recv_sem=s2_recv.at[it, d], device_id=(row, lax.rem(col + d, n_col)), device_id_type=MESH)
            for d in range(1, n_col)
        ]
        for copy in twos:
            copy.start()
        cs_wait()

        def make_image(i, carry):
            rows = pl.ds(pl.multiple_of(h + i * 32, 32), 32)
            near = pl.ds(pl.multiple_of(i * 32, 32), 32)
            G[:, rows, h:2 * h] = S[:, rows, h:2 * h] + CB[1, :, near, :] + RIDGE * R[:, rows, h:2 * h]
            G[:, rows, 2 * h:3 * h] = S[:, rows, 2 * h:3 * h] + CB[0, :, near, :] + RIDGE * R[:, rows, 2 * h:3 * h]
            return carry
        lax.fori_loop(0, side // 32, make_image, 0)
        gather_wait = None if last else gather()
        for copy in twos:
            copy.wait()
        total = T2[it, 0]
        for q in range(1, n_col):
            total = total + T2[it, q]
        rr = jnp.sum(jnp.where(ti == 0, total, 0.0), keepdims=True)
        pap = jnp.sum(jnp.where(ti == 1, total, 0.0), keepdims=True)
        if it == 0:
            ratio = None
            alpha = rr / pap
        else:
            ratio = rr / rr_before
            alpha = rr / (pap - ratio * rr / alpha)
        rr_before = rr

        def advance(i, carry):
            near = pl.ds(pl.multiple_of(i * 32, 32), 32)
            rows = pl.ds(pl.multiple_of(h + i * 32, 32), 32)
            for c in range(2):
                r = R[c, rows, own]
                d = r if it == 0 else r + ratio * D[c, near, :]
                if not last:
                    D[c, near, :] = d
                sol_ref[c, near, :] = alpha * d if it == 0 else sol_ref[c, near, :] + alpha * d
                if last:
                    along = G[c, rows, own] + ratio * L[c, rows, own]
                    res_ref[c, near, :] = r - alpha * along
            return carry
        lax.fori_loop(0, side // 32, advance, 0)
        if not last:
            gather_wait()

            def advance_r(rows, _):
                for c in range(2):
                    along = G[c, rows, :] if it == 0 else G[c, rows, :] + ratio * L[c, rows, :]
                    L[c, rows, :] = along
                    R[c, rows, :] = R[c, rows, :] - alpha * along
            chunks(2 * side, 32, advance_r)


def solution(mesh):
    n_row, n_col = mesh.shape["row"], mesh.shape["col"]

    def local(right_side, probe, weights, offsets, counts):
        side = probe.shape[1]
        cap = offsets.shape[2]
        h = side // 2
        mats = jnp.asarray(tables(side))
        by_row = jnp.concatenate([weights[0::2], weights[1::2]], axis=0)
        w = jnp.stack([jnp.concatenate([by_row[:, q::2]] * 2, axis=1) for q in range(2)])
        block = jax.ShapeDtypeStruct((2, side, side), F32)
        vmem = pl.BlockSpec(memory_space=pltpu.VMEM)
        smem = pl.BlockSpec(memory_space=pltpu.SMEM)
        wide = pltpu.VMEM((2, 2 * side, 2 * side), F32)
        dma = pltpu.SemaphoreType.DMA
        return pl.pallas_call(
            functools.partial(kernel, n_row, n_col, cap, side),
            out_shape=(block, block),
            in_specs=[smem, smem, vmem, vmem, vmem, vmem],
            out_specs=(vmem, vmem),
            scratch_shapes=[
                wide, wide, wide, wide,
                pltpu.VMEM((2, side, side), F32),
                pltpu.VMEM((cap, 2, side, side), F32),
                pltpu.VMEM((4, 2, side, side), BF16),
                pltpu.VMEM((4, side, side), F32),
                pltpu.VMEM((2, 2, h, 2 * side), F32),
                pltpu.VMEM((2, 2, side, h), F32),
                pltpu.VMEM((8, 128), F32),
                pltpu.VMEM((ITERS, n_row, 8, 128), F32),
                pltpu.VMEM((ITERS, n_col, 8, 128), F32),
                dma((8,)), dma((8,)),
                dma((ITERS, n_row)), dma((ITERS, n_row)),
                dma((ITERS, n_col)), dma((ITERS, n_col)),
            ],
            compiler_params=pltpu.CompilerParams(
                collective_id=0, has_side_effects=True, vmem_limit_bytes=48 * 1024 * 1024),
        )(offsets.reshape(-1), counts.reshape(-1), right_side, probe, w, mats)

    placed = (P(None, "row", "col"), P(), P(), P("row", "col", None, None), P("row", "col"))
    return jax.shard_map(
        local, mesh=mesh, in_specs=placed, out_specs=(P(None, "row", "col"), P(None, "row", "col")), check_vma=False)
```

```python
import functools
import math

import jax
import jax.numpy as jnp
import numpy as np
from jax import lax
from jax.experimental import pallas as pl
from jax.experimental.pallas import tpu as pltpu
from jax.sharding import PartitionSpec as P

ITERS = 3
RIDGE = 0.5
MESH = pl.DeviceIdType.MESH
F32 = jnp.float32
BF16 = jnp.bfloat16


def tables(length):
    half = length // 2
    k = np.arange(half)[:, None]
    n = np.arange(half)[None, :]
    out = []
    for odd in (0, 1):
        angle = 2.0 * math.pi * ((n * (2 * k + odd)) % length) / length
        re, im = np.cos(angle) / math.sqrt(length), -np.sin(angle) / math.sqrt(length)
        real = np.block([[re, -im], [im, re]])
        for mat in (real, real.T):
            hi = mat.astype(BF16)
            out += [hi, (mat - hi.astype(np.float64)).astype(BF16)]
    return np.stack(out)


def kernel(
    n_row, n_col, cap, side,
    off_ref, cnt_ref, rhs_ref, probe_ref, w_ref, mat_ref,
    sol_ref, res_ref,
    R, G, L, S, D, PR, X, Y, W, RA, CA, CC, RC, T1, T2,
    bar_send, bar_recv, s1_send, s1_recv, s2_send, s2_recv,
):
    h = side // 2
    own = slice(h, h + side)
    row = lax.axis_index("row")
    col = lax.axis_index("col")

    def chunks(total, step, body):
        def run(i, carry):
            body(pl.ds(pl.multiple_of(i * step, step), step), i * step)
            return carry
        lax.fori_loop(0, total // step, run, 0)

    def clear(rows, _):
        G[:, rows, :] = jnp.zeros((2, 32, 2 * side), F32)
    chunks(2 * side, 32, clear)

    for buf in (RA, CA, CC, RC):
        def clear_b(rows, _, buf=buf):
            buf[:, rows, :] = jnp.zeros((2, 32, buf.shape[2]), F32)
        chunks(buf.shape[1], 32, clear_b)
    G[:, own, own] = rhs_ref[...]

    barrier = pltpu.get_barrier_semaphore()
    for d in range(1, n_row):
        pl.semaphore_signal(barrier, inc=1, device_id=(lax.rem(row + d, n_row), col), device_id_type=MESH)
    for d in range(1, n_col):
        pl.semaphore_signal(barrier, inc=1, device_id=(row, lax.rem(col + d, n_col)), device_id_type=MESH)
    pl.semaphore_wait(barrier, n_row - 1 + n_col - 1)

    def both(index, low_src, low_dst, high_src, high_dst, axis):
        at, count = (row, n_row) if axis == 0 else (col, n_col)

        def target(step):
            return (row + step, col) if axis == 0 else (row, col + step)

        low = pltpu.make_async_remote_copy(
            src_ref=low_src, dst_ref=low_dst, send_sem=bar_send.at[2 * index], recv_sem=bar_recv.at[2 * index],
            device_id=target(-1), device_id_type=MESH)
        high = pltpu.make_async_remote_copy(
            src_ref=high_src, dst_ref=high_dst, send_sem=bar_send.at[2 * index + 1],
            recv_sem=bar_recv.at[2 * index + 1], device_id=target(1), device_id_type=MESH)

        def start():
            pl.when(at > 0)(low.start)
            pl.when(at < count - 1)(high.start)

        def wait():
            @pl.when(at > 0)
            def _():
                low.wait_send()
                high.wait_recv()

            @pl.when(at < count - 1)
            def _():
                high.wait_send()
                low.wait_recv()

        return start, wait

    def gather():
        re_start, re_wait = both(
            4, G.at[0, own, h:2 * h], G.at[0, own, 3 * h:4 * h], G.at[0, own, 2 * h:3 * h], G.at[0, own, 0:h], 1)
        im_start, im_wait = both(
            5, G.at[1, h:2 * h, own], G.at[1, 3 * h:4 * h, own], G.at[1, 2 * h:3 * h, own], G.at[1, 0:h, own], 0)
        re_start()
        im_start()
        re_wait()
        re_start, re_wait = both(
            6, G.at[0, h:2 * h, :], G.at[0, 3 * h:4 * h, :], G.at[0, 2 * h:3 * h, :], G.at[0, 0:h, :], 0)
        re_start()
        im_wait()
        im_start, im_wait = both(
            7, G.at[1, :, h:2 * h], G.at[1, :, 3 * h:4 * h], G.at[1, :, 2 * h:3 * h], G.at[1, :, 0:h], 1)
        im_start()

        def wait():
            re_wait()
            im_wait()

        return wait

    gather_wait = gather()

    for s in range(cap):
        on = jnp.where(s < cnt_ref[0], 1.0, 0.0).astype(F32)
        for c in range(2):
            rolled = pltpu.roll(probe_ref[c], off_ref[2 * s] + h, 0)
            PR[s, c] = pltpu.roll(rolled, off_ref[2 * s + 1] + h, 1) * on

    def three(val):
        top = val.astype(BF16)
        rest = val - top.astype(F32)
        mid = rest.astype(BF16)
        return top, mid, (rest - mid.astype(F32)).astype(BF16)

    first = lax.broadcasted_iota(jnp.int32, (side, side), 0)
    second = lax.broadcasted_iota(jnp.int32, (side, side), 1)
    freq = jnp.where(first >= h, 2 * (first - h) + 1, 2 * first)
    pick = jnp.where(second == freq, 1.0, 0.0).astype(BF16)
    by_row = sum(jnp.dot(pick, part, preferred_element_type=F32) for part in three(w_ref[...]))
    parts = three(by_row)
    lane = jnp.where(second >= h, second - h, second)
    for q in range(2):
        pick = jnp.where(first == 2 * lane + q, 1.0, 0.0).astype(BF16)
        W[q] = sum(jnp.dot(part, pick, preferred_element_type=F32) for part in parts)

    def clear_s(rows, _):
        S[:, rows, :] = jnp.zeros((2, 32, 2 * side), F32)
    chunks(2 * side, 32, clear_s)

    gather_wait()

    def put(j, rows, val):
        hi = val.astype(BF16)
        X[j, 0, rows, :] = hi
        X[j, 1, rows, :] = (val - hi.astype(F32)).astype(BF16)

    def left(m, j):
        hi, lo = mat_ref[m], mat_ref[m + 1]
        xh, xl = X[j, 0], X[j, 1]
        return jnp.dot(jnp.concatenate([hi, lo, hi], 1), jnp.concatenate([xh, xh, xl], 0), preferred_element_type=F32)

    def right(j, m):
        hi, lo = mat_ref[m], mat_ref[m + 1]
        xh, xl = X[j, 0], X[j, 1]
        return jnp.dot(jnp.concatenate([xh, xl, xh], 1), jnp.concatenate([hi, hi, lo], 0), preferred_element_type=F32)

    step = 32

    def fold(val):
        return jnp.sum(val.reshape(-1, 8, val.shape[-1]), axis=0)

    def patch(s, acc):
        a = off_ref[2 * s] + h
        b = off_ref[2 * s + 1] + h
        ri = lax.broadcasted_iota(jnp.int32, (step, side), 0)
        in_col = lax.broadcasted_iota(jnp.int32, (step, side), 1) >= b
        for t in range(0, h, step):
            parts = []
            for base in (t, h + t):
                rows, far = slice(base, base + step), slice(side + base, side + base + step)
                in_row = ri + base >= a
                v = [
                    jnp.where(in_row, jnp.where(in_col, R[c, rows, 0:side], R[c, rows, side:]),
                              jnp.where(in_col, R[c, far, 0:side], R[c, far, side:]))
                    for c in range(2)
                ]
                p0, p1 = PR[s, 0, rows, :], PR[s, 1, rows, :]
                parts.append((p0 * v[0] - p1 * v[1], p0 * v[1] + p1 * v[0]))
            for c in range(2):
                rows = slice(c * h + t, c * h + t + step)
                put(0, rows, parts[0][c] + parts[1][c])
                put(1, rows, parts[0][c] - parts[1][c])
        Y[0] = left(0, 0)
        Y[1] = left(4, 1)
        for j in range(2):
            for t in range(0, h, step):
                re, im = Y[j, t:t + step, :], Y[j, h + t:h + t + step, :]
                rows = slice(j * h + t, j * h + t + step)
                put(2, rows, jnp.concatenate([re[:, :h] + re[:, h:], im[:, :h] + im[:, h:]], 1))
                put(3, rows, jnp.concatenate([re[:, :h] - re[:, h:], im[:, :h] - im[:, h:]], 1))
        Y[2] = right(2, 2)
        Y[3] = right(3, 6)
        for j in range(2):
            for t in range(0, side, step):
                rows = slice(t, t + step)
                f = Y[2 + j, rows, :]
                wf = W[j, rows, :] * f
                acc = acc + fold(wf * f)
                put(j, rows, wf)
        Y[0] = right(0, 0)
        Y[1] = right(1, 4)
        for j in range(2):
            for t in range(0, h, step):
                rows = slice(j * h + t, j * h + t + step)
                c, d = Y[0, rows, :], Y[1, rows, :]
                p, m = c + d, c - d
                put(2 + j, slice(t, t + step), jnp.concatenate([p[:, :h], m[:, :h]], 1))
                put(2 + j, slice(h + t, h + t + step), jnp.concatenate([p[:, h:], m[:, h:]], 1))
        Y[2] = left(2, 2)
        Y[3] = left(6, 3)
        for t in range(0, h, step):
            for sign, base in ((1, t), (-1, h + t)):
                rows, far = slice(base, base + step), slice(side + base, side + base + step)
                hr = Y[2, t:t + step, :] + sign * Y[3, t:t + step, :]
                hi = Y[2, h + t:h + t + step, :] + sign * Y[3, h + t:h + t + step, :]
                p0, p1 = PR[s, 0, rows, :], PR[s, 1, rows, :]
                in_row = ri + base >= a
                for c, term in ((0, p0 * hr + p1 * hi), (1, p0 * hi - p1 * hr)):
                    near_r = jnp.where(in_row, term, 0.0)
                    far_r = term - near_r
                    nn = jnp.where(in_col, near_r, 0.0)
                    fn = jnp.where(in_col, far_r, 0.0)
                    S[c, rows, 0:side] += nn
                    S[c, rows, side:] += near_r - nn
                    S[c, far, 0:side] += fn
                    S[c, far, side:] += far_r - fn
        return acc

    def copy_r(rows, _):
        R[:, rows, :] = G[:, rows, :]
    chunks(2 * side, 32, copy_r)

    ti = lax.broadcasted_iota(jnp.int32, (8, 128), 0)

    def lanes(acc):
        total = acc[:, 0:128]
        for q in range(128, acc.shape[1], 128):
            total = total + acc[:, q:q + 128]
        return jnp.sum(total, axis=0, keepdims=True)

    alpha = rr_before = None
    for it in range(ITERS):
        last = it + 1 == ITERS

        def norm(i, acc):
            v = R[:, pl.ds(pl.multiple_of(h + i * 32, 32), 32), own]
            return acc + fold(v[0] * v[0]) + fold(v[1] * v[1])
        rr_acc = lax.fori_loop(0, side // 32, norm, jnp.zeros((8, side), F32))
        acc = lax.fori_loop(0, cap, patch, jnp.zeros((8, side), F32))

        re_start, re_wait = both(0, S.at[0, 0:h, :], RA.at[0], S.at[0, 3 * h:4 * h, :], RA.at[1], 0)
        im_start, im_wait = both(1, S.at[1, :, 0:h], CC.at[0], S.at[1, :, 3 * h:4 * h], CC.at[1], 1)
        re_start()
        im_start()
        rr_l, pap_l = lanes(rr_acc), lanes(acc)
        T1[it, row] = jnp.where(ti == 0, rr_l, jnp.where(ti == 1, pap_l + RIDGE * rr_l, 0.0))
        ones = [
            pltpu.make_async_remote_copy(
                src_ref=T1.at[it, row], dst_ref=T1.at[it, row], send_sem=s1_send.at[it, d],
                recv_sem=s1_recv.at[it, d], device_id=(lax.rem(row + d, n_row), col), device_id_type=MESH)
            for d in range(1, n_row)
        ]
        for copy in ones:
            copy.start()
        re_wait()

        def add_rows(i, carry):
            near = pl.ds(pl.multiple_of(i * 32, 32), 32)
            top = pl.ds(pl.multiple_of(h + i * 32, 32), 32)
            bottom = pl.ds(pl.multiple_of(2 * h + i * 32, 32), 32)
            S[0, top, :] += RA[1, near, :]
            S[0, bottom, :] += RA[0, near, :]
            return carry
        lax.fori_loop(0, h // 32, add_rows, 0)
        re_start, re_wait = both(2, S.at[0, own, 0:h], CA.at[0], S.at[0, own, 3 * h:4 * h], CA.at[1], 1)
        re_start()
        im_wait()

        def add_cols(rows, _):
            S[1, rows, h:2 * h] += CC[1, rows, :]
            S[1, rows, 2 * h:3 * h] += CC[0, rows, :]
        chunks(2 * side, 32, add_cols)
        im_start, im_wait = both(3, S.at[1, 0:h, own], RC.at[0], S.at[1, 3 * h:4 * h, own], RC.at[1], 0)
        im_start()
        for copy in ones:
            copy.wait()
        total = T1[it, 0]
        for q in range(1, n_row):
            total = total + T1[it, q]
        T2[it, col] = total
        twos = [
            pltpu.make_async_remote_copy(
                src_ref=T2.at[it, col], dst_ref=T2.at[it, col], send_sem=s2_send.at[it, d],
                recv_sem=s2_recv.at[it, d], device_id=(row, lax.rem(col + d, n_col)), device_id_type=MESH)
            for d in range(1, n_col)
        ]
        for copy in twos:
            copy.start()
        re_wait()

        def make_re(i, carry):
            rows = pl.ds(pl.multiple_of(h + i * 32, 32), 32)
            near = pl.ds(pl.multiple_of(i * 32, 32), 32)
            G[0, rows, h:2 * h] = S[0, rows, h:2 * h] + CA[1, near, :] + RIDGE * R[0, rows, h:2 * h]
            G[0, rows, 2 * h:3 * h] = S[0, rows, 2 * h:3 * h] + CA[0, near, :] + RIDGE * R[0, rows, 2 * h:3 * h]
            return carry
        lax.fori_loop(0, side // 32, make_re, 0)
        im_wait()

        def make_im(i, carry):
            near = pl.ds(pl.multiple_of(i * 32, 32), 32)
            for q in range(2):
                rows = pl.ds(pl.multiple_of((1 + q) * h + i * 32, 32), 32)
                G[1, rows, own] = S[1, rows, own] + RC[1 - q, near, :] + RIDGE * R[1, rows, own]
            return carry
        lax.fori_loop(0, h // 32, make_im, 0)
        gather_wait = None if last else gather()
        for copy in twos:
            copy.wait()
        total = T2[it, 0]
        for q in range(1, n_col):
            total = total + T2[it, q]
        rr = jnp.sum(jnp.where(ti == 0, total, 0.0), keepdims=True)
        pap = jnp.sum(jnp.where(ti == 1, total, 0.0), keepdims=True)
        if it == 0:
            ratio = None
            alpha = rr / pap
        else:
            ratio = rr / rr_before
            alpha = rr / (pap - ratio * rr / alpha)
        rr_before = rr

        def advance(i, carry):
            near = pl.ds(pl.multiple_of(i * 32, 32), 32)
            rows = pl.ds(pl.multiple_of(h + i * 32, 32), 32)
            for c in range(2):
                r = R[c, rows, own]
                d = r if it == 0 else r + ratio * D[c, near, :]
                if not last:
                    D[c, near, :] = d
                sol_ref[c, near, :] = alpha * d if it == 0 else sol_ref[c, near, :] + alpha * d
                if last:
                    along = G[c, rows, own] + ratio * L[c, rows, own]
                    res_ref[c, near, :] = r - alpha * along
            return carry
        lax.fori_loop(0, side // 32, advance, 0)
        if not last:
            chunks(2 * side, 32, clear_s)
            gather_wait()

            def advance_r(rows, _):
                for c in range(2):
                    along = G[c, rows, :] if it == 0 else G[c, rows, :] + ratio * L[c, rows, :]
                    L[c, rows, :] = along
                    R[c, rows, :] = R[c, rows, :] - alpha * along
            chunks(2 * side, 32, advance_r)


def solution(mesh):
    n_row, n_col = mesh.shape["row"], mesh.shape["col"]

    def local(right_side, probe, weights, offsets, counts):
        side = probe.shape[1]
        cap = offsets.shape[2]
        h = side // 2
        mats = jnp.asarray(tables(side))
        block = jax.ShapeDtypeStruct((2, side, side), F32)
        vmem = pl.BlockSpec(memory_space=pltpu.VMEM)
        smem = pl.BlockSpec(memory_space=pltpu.SMEM)
        wide = pltpu.VMEM((2, 2 * side, 2 * side), F32)
        dma = pltpu.SemaphoreType.DMA
        return pl.pallas_call(
            functools.partial(kernel, n_row, n_col, cap, side),
            out_shape=(block, block),
            in_specs=[smem, smem, vmem, vmem, vmem, vmem],
            out_specs=(vmem, vmem),
            scratch_shapes=[
                wide, wide, wide, wide,
                pltpu.VMEM((2, side, side), F32),
                pltpu.VMEM((cap, 2, side, side), F32),
                pltpu.VMEM((4, 2, side, side), BF16),
                pltpu.VMEM((4, side, side), F32),
                pltpu.VMEM((2, side, side), F32),
                pltpu.VMEM((2, h, 2 * side), F32),
                pltpu.VMEM((2, side, h), F32),
                pltpu.VMEM((2, 2 * side, h), F32),
                pltpu.VMEM((2, h, side), F32),
                pltpu.VMEM((ITERS, n_row, 8, 128), F32),
                pltpu.VMEM((ITERS, n_col, 8, 128), F32),
                dma((16,)), dma((16,)),
                dma((ITERS, n_row)), dma((ITERS, n_row)),
                dma((ITERS, n_col)), dma((ITERS, n_col)),
            ],
            compiler_params=pltpu.CompilerParams(
                collective_id=0, has_side_effects=True, vmem_limit_bytes=48 * 1024 * 1024),
        )(offsets.reshape(-1), counts.reshape(-1), right_side, probe, weights, mats)

    placed = (P(None, "row", "col"), P(), P(), P("row", "col", None, None), P("row", "col"))
    return jax.shard_map(
        local, mesh=mesh, in_specs=placed, out_specs=(P(None, "row", "col"), P(None, "row", "col")), check_vma=False)
```

```python
import functools
import math

import jax
import jax.numpy as jnp
import numpy as np
from jax import lax
from jax.experimental import pallas as pl
from jax.experimental.pallas import tpu as pltpu
from jax.sharding import PartitionSpec as P

ITERS = 3
RIDGE = 0.5
MESH = pl.DeviceIdType.MESH
F32 = jnp.float32
BF16 = jnp.bfloat16


def tables(length):
    half = length // 2
    k = np.arange(half)[:, None]
    n = np.arange(half)[None, :]
    out = []
    for odd in (0, 1):
        angle = 2.0 * math.pi * ((n * (2 * k + odd)) % length) / length
        re, im = np.cos(angle) / math.sqrt(length), -np.sin(angle) / math.sqrt(length)
        real = np.block([[re, -im], [im, re]])
        for mat in (real, real.T):
            hi = mat.astype(BF16)
            out += [hi, (mat - hi.astype(np.float64)).astype(BF16)]
    return np.stack(out)


def kernel(
    n_row, n_col, cap, side,
    off_ref, cnt_ref, rhs_ref, probe_ref, w_ref, mat_ref,
    sol_ref, res_ref,
    R, G, L, S, D, PR, X, Y, W, RA, CA, CC, RC, T1, T2,
    bar_send, bar_recv, s1_send, s1_recv, s2_send, s2_recv,
):
    h = side // 2
    own = slice(h, h + side)
    row = lax.axis_index("row")
    col = lax.axis_index("col")

    def chunks(total, step, body):
        def run(i, carry):
            body(pl.ds(pl.multiple_of(i * step, step), step), i * step)
            return carry
        lax.fori_loop(0, total // step, run, 0)

    def clear(rows, _):
        G[:, rows, :] = jnp.zeros((2, 32, 2 * side), F32)
    chunks(2 * side, 32, clear)

    for buf in (RA, CA, CC, RC):
        def clear_b(rows, _, buf=buf):
            buf[:, rows, :] = jnp.zeros((2, 32, buf.shape[2]), F32)
        chunks(buf.shape[1], 32, clear_b)
    G[:, own, own] = rhs_ref[...]

    barrier = pltpu.get_barrier_semaphore()
    for d in range(1, n_row):
        pl.semaphore_signal(barrier, inc=1, device_id=(lax.rem(row + d, n_row), col), device_id_type=MESH)
    for d in range(1, n_col):
        pl.semaphore_signal(barrier, inc=1, device_id=(row, lax.rem(col + d, n_col)), device_id_type=MESH)
    pl.semaphore_wait(barrier, n_row - 1 + n_col - 1)

    def both(index, low_src, low_dst, high_src, high_dst, axis):
        at, count = (row, n_row) if axis == 0 else (col, n_col)

        def target(step):
            return (row + step, col) if axis == 0 else (row, col + step)

        low = pltpu.make_async_remote_copy(
            src_ref=low_src, dst_ref=low_dst, send_sem=bar_send.at[2 * index], recv_sem=bar_recv.at[2 * index],
            device_id=target(-1), device_id_type=MESH)
        high = pltpu.make_async_remote_copy(
            src_ref=high_src, dst_ref=high_dst, send_sem=bar_send.at[2 * index + 1],
            recv_sem=bar_recv.at[2 * index + 1], device_id=target(1), device_id_type=MESH)

        def start():
            pl.when(at > 0)(low.start)
            pl.when(at < count - 1)(high.start)

        def wait():
            @pl.when(at > 0)
            def _():
                low.wait_send()
                high.wait_recv()

            @pl.when(at < count - 1)
            def _():
                high.wait_send()
                low.wait_recv()

        return start, wait

    edges = (slice(0, h), slice(3 * h, 4 * h))
    one, two, top_h, end_h = slice(h, 2 * h), slice(2 * h, 3 * h), slice(0, h), slice(3 * h, 4 * h)

    def gather():
        re_turn = both(8, G.at[0, own, one], G.at[0, own, end_h], G.at[0, own, two], G.at[0, own, top_h], 1)
        im_turn = both(9, G.at[1, one, own], G.at[1, end_h, own], G.at[1, two, own], G.at[1, top_h, own], 0)
        rest = [
            both(10, G.at[0, one, own], G.at[0, end_h, own], G.at[0, two, own], G.at[0, top_h, own], 0),
            both(11, G.at[1, own, one], G.at[1, own, end_h], G.at[1, own, two], G.at[1, own, top_h], 1),
        ]
        for start, _ in (re_turn, im_turn, *rest):
            start()
        re_turn[1]()
        for q, e in enumerate(edges):
            rest.append(both(12 + q, G.at[0, one, e], G.at[0, end_h, e], G.at[0, two, e], G.at[0, top_h, e], 0))
            rest[-1][0]()
        im_turn[1]()
        for q, e in enumerate(edges):
            rest.append(both(14 + q, G.at[1, e, one], G.at[1, e, end_h], G.at[1, e, two], G.at[1, e, top_h], 1))
            rest[-1][0]()

        def wait():
            for _, done in rest:
                done()

        return wait

    gather_wait = gather()

    for s in range(cap):
        on = jnp.where(s < cnt_ref[0], 1.0, 0.0).astype(F32)
        for c in range(2):
            rolled = pltpu.roll(probe_ref[c], off_ref[2 * s] + h, 0)
            PR[s, c] = pltpu.roll(rolled, off_ref[2 * s + 1] + h, 1) * on

    def three(val):
        top = val.astype(BF16)
        rest = val - top.astype(F32)
        mid = rest.astype(BF16)
        return top, mid, (rest - mid.astype(F32)).astype(BF16)

    first = lax.broadcasted_iota(jnp.int32, (side, side), 0)
    second = lax.broadcasted_iota(jnp.int32, (side, side), 1)
    freq = jnp.where(first >= h, 2 * (first - h) + 1, 2 * first)
    pick = jnp.where(second == freq, 1.0, 0.0).astype(BF16)
    by_row = sum(jnp.dot(pick, part, preferred_element_type=F32) for part in three(w_ref[...]))
    parts = three(by_row)
    lane = jnp.where(second >= h, second - h, second)
    for q in range(2):
        pick = jnp.where(first == 2 * lane + q, 1.0, 0.0).astype(BF16)
        W[q] = sum(jnp.dot(part, pick, preferred_element_type=F32) for part in parts)

    def clear_s(rows, _):
        S[:, rows, :] = jnp.zeros((2, 32, 2 * side), F32)
    chunks(2 * side, 32, clear_s)

    gather_wait()

    def put(j, rows, val):
        hi = val.astype(BF16)
        X[j, 0, rows, :] = hi
        X[j, 1, rows, :] = (val - hi.astype(F32)).astype(BF16)

    def left(m, j):
        hi, lo = mat_ref[m], mat_ref[m + 1]
        xh, xl = X[j, 0], X[j, 1]
        return jnp.dot(jnp.concatenate([hi, lo, hi], 1), jnp.concatenate([xh, xh, xl], 0), preferred_element_type=F32)

    def right(j, m):
        hi, lo = mat_ref[m], mat_ref[m + 1]
        xh, xl = X[j, 0], X[j, 1]
        return jnp.dot(jnp.concatenate([xh, xl, xh], 1), jnp.concatenate([hi, hi, lo], 0), preferred_element_type=F32)

    step = 32

    def fold(val):
        return jnp.sum(val.reshape(-1, 8, val.shape[-1]), axis=0)

    def patch(s, acc):
        a = off_ref[2 * s] + h
        b = off_ref[2 * s + 1] + h
        ri = lax.broadcasted_iota(jnp.int32, (step, side), 0)
        in_col = lax.broadcasted_iota(jnp.int32, (step, side), 1) >= b
        for t in range(0, h, step):
            parts = []
            for base in (t, h + t):
                rows, far = slice(base, base + step), slice(side + base, side + base + step)
                in_row = ri + base >= a
                v = [
                    jnp.where(in_row, jnp.where(in_col, R[c, rows, 0:side], R[c, rows, side:]),
                              jnp.where(in_col, R[c, far, 0:side], R[c, far, side:]))
                    for c in range(2)
                ]
                p0, p1 = PR[s, 0, rows, :], PR[s, 1, rows, :]
                parts.append((p0 * v[0] - p1 * v[1], p0 * v[1] + p1 * v[0]))
            for c in range(2):
                rows = slice(c * h + t, c * h + t + step)
                put(0, rows, parts[0][c] + parts[1][c])
                put(1, rows, parts[0][c] - parts[1][c])
        Y[0] = left(0, 0)
        Y[1] = left(4, 1)
        for j in range(2):
            for t in range(0, h, step):
                re, im = Y[j, t:t + step, :], Y[j, h + t:h + t + step, :]
                rows = slice(j * h + t, j * h + t + step)
                put(2, rows, jnp.concatenate([re[:, :h] + re[:, h:], im[:, :h] + im[:, h:]], 1))
                put(3, rows, jnp.concatenate([re[:, :h] - re[:, h:], im[:, :h] - im[:, h:]], 1))
        Y[2] = right(2, 2)
        Y[3] = right(3, 6)
        for j in range(2):
            for t in range(0, side, step):
                rows = slice(t, t + step)
                f = Y[2 + j, rows, :]
                wf = W[j, rows, :] * f
                acc = acc + fold(wf * f)
                put(j, rows, wf)
        Y[0] = right(0, 0)
        Y[1] = right(1, 4)
        for j in range(2):
            for t in range(0, h, step):
                rows = slice(j * h + t, j * h + t + step)
                c, d = Y[0, rows, :], Y[1, rows, :]
                p, m = c + d, c - d
                put(2 + j, slice(t, t + step), jnp.concatenate([p[:, :h], m[:, :h]], 1))
                put(2 + j, slice(h + t, h + t + step), jnp.concatenate([p[:, h:], m[:, h:]], 1))
        Y[2] = left(2, 2)
        Y[3] = left(6, 3)
        for t in range(0, h, step):
            for sign, base in ((1, t), (-1, h + t)):
                rows, far = slice(base, base + step), slice(side + base, side + base + step)
                hr = Y[2, t:t + step, :] + sign * Y[3, t:t + step, :]
                hi = Y[2, h + t:h + t + step, :] + sign * Y[3, h + t:h + t + step, :]
                p0, p1 = PR[s, 0, rows, :], PR[s, 1, rows, :]
                in_row = ri + base >= a
                for c, term in ((0, p0 * hr + p1 * hi), (1, p0 * hi - p1 * hr)):
                    near_r = jnp.where(in_row, term, 0.0)
                    far_r = term - near_r
                    nn = jnp.where(in_col, near_r, 0.0)
                    fn = jnp.where(in_col, far_r, 0.0)
                    S[c, rows, 0:side] += nn
                    S[c, rows, side:] += near_r - nn
                    S[c, far, 0:side] += fn
                    S[c, far, side:] += far_r - fn
        return acc

    def copy_r(rows, _):
        R[:, rows, :] = G[:, rows, :]
    chunks(2 * side, 32, copy_r)

    ti = lax.broadcasted_iota(jnp.int32, (8, 128), 0)

    def lanes(acc):
        total = acc[:, 0:128]
        for q in range(128, acc.shape[1], 128):
            total = total + acc[:, q:q + 128]
        return jnp.sum(total, axis=0, keepdims=True)

    alpha = rr_before = None
    for it in range(ITERS):
        last = it + 1 == ITERS

        def norm(i, acc):
            v = R[:, pl.ds(pl.multiple_of(h + i * 32, 32), 32), own]
            return acc + fold(v[0] * v[0]) + fold(v[1] * v[1])
        rr_acc = lax.fori_loop(0, side // 32, norm, jnp.zeros((8, side), F32))
        acc = lax.fori_loop(0, cap, patch, jnp.zeros((8, side), F32))

        re_edge = [
            both(q, S.at[0, top_h, e], RA.at[0, :, e], S.at[0, end_h, e], RA.at[1, :, e], 0)
            for q, e in enumerate(edges)
        ]
        im_edge = [
            both(2 + q, S.at[1, e, top_h], CC.at[0, e, :], S.at[1, e, end_h], CC.at[1, e, :], 1)
            for q, e in enumerate(edges)
        ]
        re_mid = both(4, S.at[0, top_h, own], RA.at[0, :, own], S.at[0, end_h, own], RA.at[1, :, own], 0)
        im_mid = both(5, S.at[1, own, top_h], CC.at[0, own, :], S.at[1, own, end_h], CC.at[1, own, :], 1)
        for start, _ in (*re_edge, *im_edge, re_mid, im_mid):
            start()
        rr_l, pap_l = lanes(rr_acc), lanes(acc)
        T1[it, row] = jnp.where(ti == 0, rr_l, jnp.where(ti == 1, pap_l + RIDGE * rr_l, 0.0))
        ones = [
            pltpu.make_async_remote_copy(
                src_ref=T1.at[it, row], dst_ref=T1.at[it, row], send_sem=s1_send.at[it, d],
                recv_sem=s1_recv.at[it, d], device_id=(lax.rem(row + d, n_row), col), device_id_type=MESH)
            for d in range(1, n_row)
        ]
        for copy in ones:
            copy.start()
        for _, done in re_edge:
            done()

        def add_rows(i, carry):
            near = pl.ds(pl.multiple_of(i * 32, 32), 32)
            for q in range(2):
                rows = pl.ds(pl.multiple_of((1 + q) * h + i * 32, 32), 32)
                for e in edges:
                    S[0, rows, e] += RA[1 - q, near, e]
            return carry
        lax.fori_loop(0, h // 32, add_rows, 0)
        re_turn = both(6, S.at[0, own, top_h], CA.at[0], S.at[0, own, end_h], CA.at[1], 1)
        re_turn[0]()
        for _, done in im_edge:
            done()

        def add_cols(i, carry):
            for base in (0, 3 * h):
                rows = pl.ds(pl.multiple_of(base + i * 32, 32), 32)
                S[1, rows, one] += CC[1, rows, :]
                S[1, rows, two] += CC[0, rows, :]
            return carry
        lax.fori_loop(0, h // 32, add_cols, 0)
        im_turn = both(7, S.at[1, top_h, own], RC.at[0], S.at[1, end_h, own], RC.at[1], 0)
        im_turn[0]()
        for copy in ones:
            copy.wait()
        total = T1[it, 0]
        for q in range(1, n_row):
            total = total + T1[it, q]
        T2[it, col] = total
        twos = [
            pltpu.make_async_remote_copy(
                src_ref=T2.at[it, col], dst_ref=T2.at[it, col], send_sem=s2_send.at[it, d],
                recv_sem=s2_recv.at[it, d], device_id=(row, lax.rem(col + d, n_col)), device_id_type=MESH)
            for d in range(1, n_col)
        ]
        for copy in twos:
            copy.start()
        re_mid[1]()
        im_mid[1]()
        re_turn[1]()
        im_turn[1]()

        def make(i, carry):
            near = pl.ds(pl.multiple_of(i * 32, 32), 32)
            for q in range(2):
                rows = pl.ds(pl.multiple_of((1 + q) * h + i * 32, 32), 32)
                inner = pl.ds(pl.multiple_of(q * h + i * 32, 32), 32)
                re = S[0, rows, own] + RA[1 - q, near, own] + RIDGE * R[0, rows, own]
                im = S[1, rows, own] + RC[1 - q, near, :] + RIDGE * R[1, rows, own]
                G[0, rows, one] = re[:, :h] + CA[1, inner, :]
                G[0, rows, two] = re[:, h:] + CA[0, inner, :]
                G[1, rows, one] = im[:, :h] + CC[1, rows, :]
                G[1, rows, two] = im[:, h:] + CC[0, rows, :]
            return carry
        lax.fori_loop(0, h // 32, make, 0)
        gather_wait = None if last else gather()
        for copy in twos:
            copy.wait()
        total = T2[it, 0]
        for q in range(1, n_col):
            total = total + T2[it, q]
        rr = jnp.sum(jnp.where(ti == 0, total, 0.0), keepdims=True)
        pap = jnp.sum(jnp.where(ti == 1, total, 0.0), keepdims=True)
        if it == 0:
            ratio = None
            alpha = rr / pap
        else:
            ratio = rr / rr_before
            alpha = rr / (pap - ratio * rr / alpha)
        rr_before = rr

        def advance(i, carry):
            near = pl.ds(pl.multiple_of(i * 32, 32), 32)
            rows = pl.ds(pl.multiple_of(h + i * 32, 32), 32)
            for c in range(2):
                r = R[c, rows, own]
                d = r if it == 0 else r + ratio * D[c, near, :]
                if not last:
                    D[c, near, :] = d
                sol_ref[c, near, :] = alpha * d if it == 0 else sol_ref[c, near, :] + alpha * d
                if last:
                    along = G[c, rows, own] + ratio * L[c, rows, own]
                    res_ref[c, near, :] = r - alpha * along
            return carry
        lax.fori_loop(0, side // 32, advance, 0)
        if not last:
            chunks(2 * side, 32, clear_s)
            gather_wait()

            def advance_r(rows, _):
                for c in range(2):
                    along = G[c, rows, :] if it == 0 else G[c, rows, :] + ratio * L[c, rows, :]
                    L[c, rows, :] = along
                    R[c, rows, :] = R[c, rows, :] - alpha * along
            chunks(2 * side, 32, advance_r)


def solution(mesh):
    n_row, n_col = mesh.shape["row"], mesh.shape["col"]

    def local(right_side, probe, weights, offsets, counts):
        side = probe.shape[1]
        cap = offsets.shape[2]
        h = side // 2
        mats = jnp.asarray(tables(side))
        block = jax.ShapeDtypeStruct((2, side, side), F32)
        vmem = pl.BlockSpec(memory_space=pltpu.VMEM)
        smem = pl.BlockSpec(memory_space=pltpu.SMEM)
        wide = pltpu.VMEM((2, 2 * side, 2 * side), F32)
        dma = pltpu.SemaphoreType.DMA
        return pl.pallas_call(
            functools.partial(kernel, n_row, n_col, cap, side),
            out_shape=(block, block),
            in_specs=[smem, smem, vmem, vmem, vmem, vmem],
            out_specs=(vmem, vmem),
            scratch_shapes=[
                wide, wide, wide, wide,
                pltpu.VMEM((2, side, side), F32),
                pltpu.VMEM((cap, 2, side, side), F32),
                pltpu.VMEM((4, 2, side, side), BF16),
                pltpu.VMEM((4, side, side), F32),
                pltpu.VMEM((2, side, side), F32),
                pltpu.VMEM((2, h, 2 * side), F32),
                pltpu.VMEM((2, side, h), F32),
                pltpu.VMEM((2, 2 * side, h), F32),
                pltpu.VMEM((2, h, side), F32),
                pltpu.VMEM((ITERS, n_row, 8, 128), F32),
                pltpu.VMEM((ITERS, n_col, 8, 128), F32),
                dma((32,)), dma((32,)),
                dma((ITERS, n_row)), dma((ITERS, n_row)),
                dma((ITERS, n_col)), dma((ITERS, n_col)),
            ],
            compiler_params=pltpu.CompilerParams(
                collective_id=0, has_side_effects=True, vmem_limit_bytes=48 * 1024 * 1024),
        )(offsets.reshape(-1), counts.reshape(-1), right_side, probe, weights, mats)

    placed = (P(None, "row", "col"), P(), P(), P("row", "col", None, None), P("row", "col"))
    return jax.shard_map(
        local, mesh=mesh, in_specs=placed, out_specs=(P(None, "row", "col"), P(None, "row", "col")), check_vma=False)
```
